32 devices in a mesh: model: 4 (over z), data: 2 (over y), stage: 4 (over x, core).
Axes of the slice: x: 2, y: 2, z: 4, core: 2. Of those that a mesh axis runs over, the one named last changes fastest.
Arguments:
- w_up: float32 [4, 1024, 4096], P('stage', None, 'model')
- w_down: float32 [4, 4096, 1024], P('stage', 'model')
- m_up: float32 [4, 1024, 4096], P('stage', None, 'model')
- m_down: float32 [4, 4096, 1024], P('stage', 'model')
- v_up: float32 [4, 1024, 4096], P('stage', None, 'model')
- v_down: float32 [4, 4096, 1024], P('stage', 'model')
- g_up: float32 [2, 4, 1024, 4096], P('data', 'stage', None, 'model')
- g_down: float32 [2, 4, 4096, 1024], P('data', 'stage', 'model')
- acts_last: bfloat16 [4, 256, 1024], P('stage', 'data')
- grad_out: bfloat16 [256, 1024], P('data')
- x_next: bfloat16 [3, 256, 1024], P(None, 'data')
- learn_rate: float32 [1], replicated
- max_norm: float32 [1], replicated
Outputs:
- output 1: float32 [4, 1024, 4096], P('stage', None, 'model')
- output 2: float32 [4, 4096, 1024], P('stage', 'model')
- output 3: float32 [4, 1024, 4096], P('stage', None, 'model')
- output 4: float32 [4, 4096, 1024], P('stage', 'model')
- output 5: float32 [4, 1024, 4096], P('stage', None, 'model')
- output 6: float32 [4, 4096, 1024], P('stage', 'model')
- output 7: bfloat16 [3, 256, 1024], P(None, 'data')
All inputs are finite; a program needn't handle non-finite values.
Results may differ from the reference program's by a relative error of at most 0.00840855.
Values are sent between devices in bfloat16 or wider.
A program may use at most 1 GiB of HBM per device.

```python
import jax
import jax.numpy as jnp
from jax import lax

STAGES = 4
REPLICAS = 2
D_MODEL = 1024
FF_WIDTH = 4096
MICRO_ROWS = 128
NEXT_MICRO = 3
ADAM_STEP = 10
BETA_ONE = 0.9
BETA_TWO = 0.95
ADAM_EPS = 1e-8
WEIGHT_DECAY = 0.1
NORM_EPS = 1e-6
ALL_ROWS = REPLICAS * MICRO_ROWS


def gelu_vjp(pre_act, upstream):
    pull_back = jax.vjp(jax.nn.gelu, pre_act)[1]
    return pull_back(upstream)[0]


def stage_apply(acts_in, up_bf, down_bf):
    pre_act = jnp.dot(acts_in, up_bf, preferred_element_type=jnp.float32)
    hidden = jax.nn.gelu(pre_act).astype(jnp.bfloat16)
    branch = jnp.dot(hidden, down_bf, preferred_element_type=jnp.float32)
    return (acts_in.astype(jnp.float32) + branch).astype(jnp.bfloat16)


def averaged_grads(w_up, w_down, g_up, g_down, acts_last, grad_out):
    def back_step(upstream, layer_in):
        up_bf, down_bf, acts_in = layer_in
        pre_act = jnp.dot(acts_in, up_bf, preferred_element_type=jnp.float32)
        hidden = jax.nn.gelu(pre_act).astype(jnp.bfloat16)
        grad_down = jnp.dot(hidden.T, upstream, preferred_element_type=jnp.float32)
        grad_hid = jnp.dot(upstream, down_bf.T, preferred_element_type=jnp.float32)
        grad_pre = gelu_vjp(pre_act, grad_hid).astype(jnp.bfloat16)
        grad_up = jnp.dot(acts_in.T, grad_pre, preferred_element_type=jnp.float32)
        back_in = jnp.dot(grad_pre, up_bf.T, preferred_element_type=jnp.float32)
        grad_in = (upstream.astype(jnp.float32) + back_in).astype(jnp.bfloat16)
        return grad_in, (grad_up, grad_down)
    layer_all = (w_up.astype(jnp.bfloat16), w_down.astype(jnp.bfloat16), acts_last)
    grad_pair = lax.scan(back_step, grad_out, layer_all, reverse=True)[1]
    mean_up = (jnp.sum(g_up, axis=0) + grad_pair[0]) / REPLICAS
    mean_down = (jnp.sum(g_down, axis=0) + grad_pair[1]) / REPLICAS
    return mean_up, mean_down


def adamw_update(weight, moment_one, moment_two, grad_step, step_rate):
    mom_new = BETA_ONE * moment_one + (1.0 - BETA_ONE) * grad_step
    sec_new = BETA_TWO * moment_two + (1.0 - BETA_TWO) * grad_step * grad_step
    one_corr = 1.0 - BETA_ONE ** ADAM_STEP
    two_corr = 1.0 - BETA_TWO ** ADAM_STEP
    direction = (mom_new / one_corr) / (jnp.sqrt(sec_new / two_corr) + ADAM_EPS)
    weight_new = weight - step_rate * (direction + WEIGHT_DECAY * weight)
    return weight_new, mom_new, sec_new


def forward_all(up_bf, down_bf, x_next):
    def one_micro(acts_in):
        def fwd_step(acts_carry, layer_in):
            return stage_apply(acts_carry, layer_in[0], layer_in[1]), None
        return lax.scan(fwd_step, acts_in, (up_bf, down_bf))[0]
    return lax.map(one_micro, x_next)


def setup_inputs(seed: int = 0) -> dict:
    key_list = jax.random.split(jax.random.key(seed), 13)
    up_scale = D_MODEL ** -0.5
    down_scale = FF_WIDTH ** -0.5
    grad_scale = MICRO_ROWS ** 0.5
    w_up = jax.random.normal(key_list[0], (STAGES, D_MODEL, FF_WIDTH), jnp.float32) * up_scale
    w_down = jax.random.normal(key_list[1], (STAGES, FF_WIDTH, D_MODEL), jnp.float32) * down_scale
    g_up = jax.random.normal(key_list[2], (REPLICAS, STAGES, D_MODEL, FF_WIDTH), jnp.float32) * (0.3 * grad_scale)
    g_down = jax.random.normal(key_list[3], (REPLICAS, STAGES, FF_WIDTH, D_MODEL), jnp.float32) * (0.5 * grad_scale)
    acts_last = jax.random.normal(key_list[4], (STAGES, ALL_ROWS, D_MODEL), jnp.float32).astype(jnp.bfloat16)
    grad_out = jax.random.normal(key_list[5], (ALL_ROWS, D_MODEL), jnp.float32).astype(jnp.bfloat16)
    x_next = jax.random.normal(key_list[6], (NEXT_MICRO, ALL_ROWS, D_MODEL), jnp.float32).astype(jnp.bfloat16)
    learn_rate = jax.random.uniform(key_list[7], (1,), jnp.float32, 0.1, 0.25) * up_scale
    mean_up, mean_down = averaged_grads(w_up, w_down, g_up, g_down, acts_last, grad_out)
    grad_norm = jnp.sqrt(jnp.sum(mean_up * mean_up) + jnp.sum(mean_down * mean_down))
    clip_frac = jax.random.uniform(key_list[8], (1,), jnp.float32, 0.35, 0.65)
    max_norm = clip_frac * grad_norm
    up_rms = clip_frac[0] * jnp.sqrt(jnp.mean(mean_up * mean_up))
    down_rms = clip_frac[0] * jnp.sqrt(jnp.mean(mean_down * mean_down))
    m_up = jax.random.normal(key_list[9], w_up.shape, jnp.float32) * (0.1 * up_rms)
    m_down = jax.random.normal(key_list[10], w_down.shape, jnp.float32) * (0.1 * down_rms)
    v_up = (0.5 + jax.random.uniform(key_list[11], w_up.shape, jnp.float32)) * (0.02 * up_rms * up_rms)
    v_down = (0.5 + jax.random.uniform(key_list[12], w_down.shape, jnp.float32)) * (0.02 * down_rms * down_rms)
    return {'w_up': w_up, 'w_down': w_down, 'm_up': m_up, 'm_down': m_down, 'v_up': v_up, 'v_down': v_down, 'g_up': g_up, 'g_down': g_down, 'acts_last': acts_last, 'grad_out': grad_out, 'x_next': x_next, 'learn_rate': learn_rate, 'max_norm': max_norm}


def reference(w_up, w_down, m_up, m_down, v_up, v_down, g_up, g_down, acts_last, grad_out, x_next, learn_rate, max_norm):
    mean_up, mean_down = averaged_grads(w_up, w_down, g_up, g_down, acts_last, grad_out)
    norm_sq = jnp.sum(mean_up * mean_up) + jnp.sum(mean_down * mean_down)
    clip_scale = jnp.minimum(1.0, max_norm[0] / (jnp.sqrt(norm_sq) + NORM_EPS))
    up_new, up_mom, up_sec = adamw_update(w_up, m_up, v_up, clip_scale * mean_up, learn_rate[0])
    down_new, down_mom, down_sec = adamw_update(w_down, m_down, v_down, clip_scale * mean_down, learn_rate[0])
    y_next = forward_all(up_new.astype(jnp.bfloat16), down_new.astype(jnp.bfloat16), x_next)
    return (up_new, down_new, up_mom, down_mom, up_sec, down_sec, y_next)
```

```python
import functools

import jax
import jax.numpy as jnp
from jax import lax
from jax.experimental import pallas as pl
from jax.experimental.pallas import tpu as pltpu
from jax.sharding import PartitionSpec as P

ADAM_STEP = 10
BETA_ONE = 0.9
BETA_TWO = 0.95
ADAM_EPS = 1e-8
WEIGHT_DECAY = 0.1
NORM_EPS = 1e-6
GELU_A = 0.7978845608028654
GELU_B = 0.044715
NT = (((1,), (1,)), ((), ()))
TN = (((0,), (0,)), ((), ()))
MESH = pl.DeviceIdType.MESH
F32 = jnp.float32
BF16 = jnp.bfloat16
NZ = 4
NS = 4
ROWS = 128
D = 1024
QROWS = ROWS // NZ
CH = 128
NCHUNK = 2 * D // CH
R = 64
RQ = R // NZ
NSUB = ROWS // R
NMICRO = 3
NF = NMICRO * 2 * NSUB
PRE = (11, 8, 5, 2)


def gelu_parts(x):
    t = jnp.tanh(GELU_A * (x + GELU_B * (x * x * x)))
    return 0.5 * (1.0 + t), t


def rcopy(src, dst, ssem, rsem, dev):
    return pltpu.make_async_remote_copy(src, dst, ssem, rsem, device_id=dev, device_id_type=MESH)


def axes():
    return lax.axis_index('model'), lax.axis_index('data'), lax.axis_index('stage')


def back_kernel(wu, wd, gu, gd, a_ref, dy_ref, x_ref, mn_ref,
                gbu, gbd, c_ref, xo_ref,
                wf, wub, wdb, gin, gown, fa, fg, fh, fz, gp, part, rsb, gsend, nacc, nsend, nbuf,
                wsem, osem, outsem, cs, cr, fs, fr, rs, rr, gs, gr, xs, xr, ys, yr, ns, nr):
    m, d, s = axes()
    prim = d == lax.rem(s, 2)
    sec = jnp.logical_not(prim)
    peer = (m, 1 - d, s)

    def chunk_copy(c, src):
        row = pl.ds(pl.multiple_of(lax.rem(c, D // CH) * CH, CH), CH)
        return rcopy(src.at[0, 0, row], gin.at[c // (D // CH), row], cs.at[c], cr.at[c], peer)

    def send_chunks(lo, hi):
        half = D // CH

        @pl.loop(lo, jnp.minimum(hi, half))
        def _(c):
            chunk_copy(c, gd).start()

        @pl.loop(jnp.maximum(lo, half), hi)
        def _(c):
            chunk_copy(c, gu).start()

    pre = jnp.where(s == 0, PRE[0], jnp.where(s == 1, PRE[1], jnp.where(s == 2, PRE[2], PRE[3])))
    own = pl.ds(0, ROWS)
    oth = pl.ds(ROWS, ROWS)
    fcopy = [rcopy(a_ref.at[0], fa.at[oth], fs.at[0], fr.at[0], peer)]
    fcopy += [rcopy(f.at[own], f.at[oth], fs.at[i + 1], fr.at[i + 1], peer) for i, f in enumerate((fh, fg, fz))]

    wcopies = [pltpu.make_async_copy(wu.at[0], wf.at[0], wsem.at[0]), pltpu.make_async_copy(wd.at[0], wf.at[1], wsem.at[1])]
    for cp in wcopies:
        cp.start()
    qrow = pl.ds(pl.multiple_of(m * QROWS, QROWS), QROWS)
    xcopy = rcopy(x_ref.at[:, qrow], xo_ref.at[:, qrow], xs.at[0], xr.at[0], (m, 0, s))

    @pl.when(sec)
    def _():
        @pl.when(s == 0)
        def _():
            xcopy.start()
        fcopy[0].start()
        send_chunks(0, pre)

    gcopies = [pltpu.make_async_copy(gd.at[0, 0], gown.at[0], osem.at[0]), pltpu.make_async_copy(gu.at[0, 0], gown.at[1], osem.at[1])]

    @pl.when(prim)
    def _():
        for cp in gcopies:
            cp.start()

    fa[own] = a_ref[0]
    for i, (cp, dst) in enumerate(zip(wcopies, (wub, wdb))):
        cp.wait()

        @pl.loop(0, D // CH)
        def _(c):
            row = pl.ds(pl.multiple_of(c * CH, CH), CH)
            dst[row] = wf[i, row].astype(BF16)
        if i == 0:
            pre_act = jnp.dot(a_ref[0], wub[...], preferred_element_type=F32)
            cdf, t = gelu_parts(pre_act)
            fh[own] = (pre_act * cdf).astype(BF16)
            gp[...] = cdf + pre_act * (0.5 * (1.0 - t * t) * GELU_A * (1.0 + 3.0 * GELU_B * (pre_act * pre_act)))

    @pl.when(sec)
    def _():
        fcopy[1].start()

    xfwd = [rcopy(xo_ref.at[:, qrow], xo_ref.at[:, qrow], ys.at[o - 1], yr.at[o - 1], (lax.rem(m + o, NZ), d, s)) for o in range(1, NZ)]

    @pl.when(jnp.logical_and(s == 0, d == 0))
    def _():
        xcopy.wait_recv()
        for cp in xfwd:
            cp.start()

    gsends = [rcopy(gsend, fg.at[qrow], gs.at[o], gr.at[o], (lax.rem(m + o, NZ), d, s - 1)) for o in range(NZ)]

    @pl.when(s == NS - 1)
    def _():
        fg[own] = dy_ref[...]

    @pl.when(s < NS - 1)
    def _():
        for cp in gsends:
            cp.wait_recv()

    @pl.when(sec)
    def _():
        fcopy[2].start()

    grad_hid = lax.dot_general(fg[own], wdb[...], NT, preferred_element_type=F32)
    fz[own] = (gp[...] * grad_hid).astype(BF16)

    @pl.when(s > 0)
    def _():
        part[...] = lax.dot_general(fz[own], wub[...], NT, preferred_element_type=F32)
        rcp = []
        for o in range(1, NZ):
            to = lax.rem(m + o, NZ)
            row = pl.ds(pl.multiple_of(to * QROWS, QROWS), QROWS)
            rcp.append(rcopy(part.at[row], rsb.at[o - 1], rs.at[o - 1], rr.at[o - 1], (to, d, s)))
        for cp in rcp:
            cp.start()
        total = part[qrow]
        for o, cp in enumerate(rcp):
            cp.wait_recv()
            total = total + rsb[o]
        gsend[...] = (fg[qrow].astype(F32) + total).astype(BF16)
        for cp in gsends:
            cp.start()
        for cp in rcp:
            cp.wait_send()

    @pl.when(sec)
    def _():
        fcopy[3].start()
        send_chunks(pre, NCHUNK)

    @pl.when(s > 0)
    def _():
        for cp in gsends:
            cp.wait_send()

    slot = s * NZ + m

    @pl.when(prim)
    def _():
        for cp in gcopies:
            cp.wait()
        for cp in fcopy:
            cp.wait_recv()
        nacc[...] = jnp.zeros_like(nacc)
        for half, (lhs, rhs, src, out) in enumerate(((fh, fg, gd, gbd), (fa, fz, gu, gbu))):
            @pl.loop(0, D // CH)
            def _(c):
                row = pl.ds(pl.multiple_of(c * CH, CH), CH)
                grad = lax.dot_general(lhs[:, row], rhs[...], TN, preferred_element_type=F32)
                chunk_copy(half * (D // CH) + c, src).wait_recv()
                bar = (gown[half, row] + gin[half, row] + grad) * 0.5
                gown[half, row] = bar
                nacc[...] += jnp.sum((bar * bar).reshape(CH // 8, 8, D), axis=0)
                pltpu.make_async_copy(gown.at[half, row], out.at[row], outsem.at[half * (D // CH) + c]).start()
        tot = nacc[:, 0:128]
        for i in range(1, D // 128):
            tot = tot + nacc[:, i * 128:(i + 1) * 128]
        nsend[...] = tot
        nbuf[slot] = tot

    def ncopy(to, sl):
        return rcopy(nsend, nbuf.at[sl], ns.at[to], nr.at[sl], (to // (2 * NS), lax.rem(to // NS, 2), lax.rem(to, NS)))

    me = (m * 2 + d) * NS + s

    @pl.when(prim)
    def _():
        @pl.loop(0, NZ * 2 * NS)
        def _(to):
            @pl.when(to != me)
            def _():
                ncopy(to, slot).start()

    @pl.loop(0, NZ * NS)
    def _(i):
        @pl.when(jnp.logical_or(sec, i != slot))
        def _():
            ncopy(0, i).wait_recv()

    total = jnp.sum(jnp.sum(nbuf[...], axis=0), keepdims=True)
    c_ref[...] = jnp.broadcast_to(jnp.minimum(1.0, mn_ref[0] / (jnp.sqrt(total) + NORM_EPS)), c_ref.shape)

    @pl.when(prim)
    def _():
        @pl.loop(0, NZ * 2 * NS)
        def _(to):
            @pl.when(to != me)
            def _():
                ncopy(to, slot).wait_send()
        for half, out in enumerate((gbd, gbu)):
            @pl.loop(0, D // CH)
            def _(c):
                row = pl.ds(pl.multiple_of(c * CH, CH), CH)
                pltpu.make_async_copy(gown.at[half, row], out.at[row], outsem.at[half * (D // CH) + c]).wait()

    @pl.when(sec)
    def _():
        for cp in fcopy:
            cp.wait_send()

        @pl.loop(0, NCHUNK)
        def _(c):
            chunk_copy(c, gd).wait_send()

    @pl.when(jnp.logical_and(s == 0, d == 0))
    def _():
        for cp in xfwd:
            cp.wait()

    @pl.when(jnp.logical_and(s == 0, d == 1))
    def _():
        xcopy.wait_send()


def fwd_kernel(w1, w2, x_ref, xo_ref, gbu_in, gbd_in, gbu, gbd, y_ref,
               inb, part, rsb, osend, isem, ir, rs, rr, os, yl, ys, yr, cs, cr):
    m, d, s = axes()
    prim = d == lax.rem(s, 2)
    sec = jnp.logical_not(prim)
    peer = (m, 1 - d, s)
    half = D // CH
    oq = pl.ds(pl.multiple_of(m * RQ, RQ), RQ)

    def bulk(c, ref):
        row = pl.ds(pl.multiple_of(lax.rem(c, half) * CH, CH), CH)
        return rcopy(ref.at[row], ref.at[row], cs.at[c], cr.at[c], peer)

    def send_chunks(lo, hi):
        @pl.loop(lo, jnp.minimum(hi, half))
        def _(c):
            bulk(c, gbd).start()

        @pl.loop(jnp.maximum(lo, half), hi)
        def _(c):
            bulk(c, gbu).start()

    up = 1 + 2 * s

    def goal(k):
        return up + (NCHUNK - up) * k // NF

    def where_is(k):
        return k // (2 * NSUB), lax.rem(k // NSUB, 2), lax.rem(k, NSUB)

    def in_copy(k, o):
        return rcopy(osend.at[k], inb.at[k, oq], os.at[k, o], ir.at[k, o], (lax.rem(m + o, NZ), lax.rem(s + 1, 2), s + 1))

    def rs_copy(k, o):
        to = lax.rem(m + o, NZ)
        row = pl.ds(pl.multiple_of(to * RQ, RQ), RQ)
        return rcopy(part.at[k, row], rsb.at[k, o - 1], rs.at[k, o - 1], rr.at[k, o - 1], (to, d, s))

    def y_place(k):
        i, r, sub = where_is(k)
        return i, r, i * NSUB + sub, pl.ds(pl.multiple_of(sub * R + m * RQ, RQ), RQ)

    def y_copy(k, o, st):
        i, r, kk, row = y_place(k)
        return rcopy(osend.at[k], y_ref.at[i, row], ys.at[k, o * NS + st], yr.at[kk, o], (lax.rem(m + o, NZ), r, st))

    def y_local(k):
        i, r, kk, row = y_place(k)
        return pltpu.make_async_copy(osend.at[k], y_ref.at[i, row], yl.at[k])

    def is_self(k, o, st):
        r = lax.rem(k // NSUB, 2)
        return jnp.logical_and(r == d, (o == 0) and (st == NS - 1))

    def compute(k):
        @pl.when(s > 0)
        def _():
            for o in range(NZ):
                in_copy(k, o).wait_recv()
        pre_act = jnp.dot(inb[k], w1[...], preferred_element_type=F32)
        hid = (pre_act * gelu_parts(pre_act)[0]).astype(BF16)
        part[k] = jnp.dot(hid, w2[...], preferred_element_type=F32)
        for o in range(1, NZ):
            rs_copy(k, o).start()

    def finish(k):
        total = part[k, oq]
        for o in range(1, NZ):
            rs_copy(k, o).wait_recv()
            total = total + rsb[k, o - 1]
        osend[k] = (inb[k, oq].astype(F32) + total).astype(BF16)

        @pl.when(s < NS - 1)
        def _():
            for o in range(NZ):
                in_copy(k, o).start()

        @pl.when(s == NS - 1)
        def _():
            for o in range(NZ):
                for st in range(NS):
                    if o == 0 and st == NS - 1:
                        @pl.when(is_self(k, o, st))
                        def _():
                            y_local(k).start()

                        @pl.when(jnp.logical_not(is_self(k, o, st)))
                        def _():
                            y_copy(k, o, st).start()
                    else:
                        y_copy(k, o, st).start()

    def in_local(k, src, row, i):
        return pltpu.make_async_copy(src.at[i, row], inb.at[k], isem.at[k])

    @pl.when(prim)
    def _():
        @pl.when(s == 0)
        def _():
            for step in ('start', 'wait'):
                for k in range(NF):
                    i, r, sub = k // (2 * NSUB), (k // NSUB) % 2, k % NSUB
                    getattr(in_local(k, (x_ref, xo_ref)[r], pl.ds(sub * R, R), i), step)()
        send_chunks(0, up)
        compute(0)

        @pl.loop(1, NF)
        def _(k):
            compute(k)
            finish(k - 1)
            send_chunks(goal(k - 1), goal(k))
        finish(NF - 1)
        send_chunks(goal(NF - 1), NCHUNK)

    @pl.loop(0, NF // 2)
    def _(kk):
        i, sub = kk // NSUB, lax.rem(kk, NSUB)
        k = i * 2 * NSUB + d * NSUB + sub
        for o in range(NZ):
            mine = jnp.logical_and(jnp.logical_and(s == NS - 1, prim), o == 0)

            @pl.when(jnp.logical_not(mine))
            def _():
                y_copy(k, o, 0).wait_recv()

            if o == 0:
                @pl.when(mine)
                def _():
                    y_local(k).wait()

    @pl.when(sec)
    def _():
        @pl.loop(0, NCHUNK)
        def _(c):
            bulk(c, gbd).wait_recv()

    @pl.when(prim)
    def _():
        @pl.loop(0, NF)
        def _(k):
            for o in range(1, NZ):
                rs_copy(k, o).wait_send()

            @pl.when(s < NS - 1)
            def _():
                for o in range(NZ):
                    in_copy(k, o).wait_send()

            @pl.when(s == NS - 1)
            def _():
                for o in range(NZ):
                    for st in range(NS):
                        if o == 0 and st == NS - 1:
                            @pl.when(jnp.logical_not(is_self(k, o, st)))
                            def _():
                                y_copy(k, o, st).wait_send()
                        else:
                            y_copy(k, o, st).wait_send()

        @pl.loop(0, NCHUNK)
        def _(c):
            bulk(c, gbd).wait_send()


def adamw_update(weight, moment_one, moment_two, grad_step, step_rate):
    mom_new = BETA_ONE * moment_one + (1.0 - BETA_ONE) * grad_step
    sec_new = BETA_TWO * moment_two + (1.0 - BETA_TWO) * grad_step * grad_step
    one_corr = 1.0 - BETA_ONE ** ADAM_STEP
    two_corr = 1.0 - BETA_TWO ** ADAM_STEP
    direction = (mom_new / one_corr) / (jnp.sqrt(sec_new / two_corr) + ADAM_EPS)
    weight_new = weight - step_rate * (direction + WEIGHT_DECAY * weight)
    return weight_new, mom_new, sec_new


def solution(mesh):
    up_spec = P('stage', None, 'model')
    down_spec = P('stage', 'model', None)
    row_spec = P(None, 'data', None)
    in_specs = (up_spec, down_spec, up_spec, down_spec, up_spec, down_spec, P('data', 'stage', None, 'model'), P('data', 'stage', 'model', None), P('stage', 'data', None), P('data', None), row_spec, P(None), P(None))
    out_specs = (up_spec, down_spec, up_spec, down_spec, up_spec, down_spec, row_spec)
    hbm = pl.BlockSpec(memory_space=pl.ANY)
    vm = pl.BlockSpec(memory_space=pltpu.VMEM)
    sm = pl.BlockSpec(memory_space=pltpu.SMEM)
    dma = pltpu.SemaphoreType.DMA
    mat = jax.ShapeDtypeStruct((D, D), F32)

    def device_step(w_up, w_down, m_up, m_down, v_up, v_down, g_up, g_down, acts_last, grad_out, x_next, learn_rate, max_norm):
        gbu, gbd, clip, x_other = pl.pallas_call(
            back_kernel,
            name='back',
            out_shape=(mat, mat, jax.ShapeDtypeStruct((8, 128), F32), jax.ShapeDtypeStruct((NMICRO, ROWS, D), BF16)),
            in_specs=[hbm, hbm, hbm, hbm, vm, vm, hbm, sm],
            out_specs=(hbm, hbm, vm, hbm),
            scratch_shapes=[
                pltpu.VMEM((2, D, D), F32), pltpu.VMEM((D, D), BF16), pltpu.VMEM((D, D), BF16),
                pltpu.VMEM((2, D, D), F32), pltpu.VMEM((2, D, D), F32),
                *[pltpu.VMEM((2 * ROWS, D), BF16)] * 4,
                pltpu.VMEM((ROWS, D), F32), pltpu.VMEM((ROWS, D), F32), pltpu.VMEM((NZ - 1, QROWS, D), F32),
                pltpu.VMEM((QROWS, D), BF16), pltpu.VMEM((8, D), F32), pltpu.VMEM((8, 128), F32), pltpu.VMEM((NZ * NS, 8, 128), F32),
                dma((2,)), dma((2,)), dma((NCHUNK,)), dma((NCHUNK,)), dma((NCHUNK,)), dma((4,)), dma((4,)),
                dma((NZ - 1,)), dma((NZ - 1,)), dma((NZ,)), dma((NZ,)), dma((1,)), dma((1,)), dma((NZ - 1,)), dma((NZ - 1,)),
                dma((NZ * 2 * NS,)), dma((NZ * NS,)),
            ],
            compiler_params=pltpu.CompilerParams(has_side_effects=True, vmem_limit_bytes=48 << 20),
        )(w_up, w_down, g_up, g_down, acts_last, grad_out, x_next, max_norm)
        clip = clip[0, 0]
        rate = learn_rate[0]
        up_bf = adamw_update(w_up[0], m_up[0], v_up[0], clip * gbu, rate)[0].astype(BF16)
        down_bf = adamw_update(w_down[0], m_down[0], v_down[0], clip * gbd, rate)[0].astype(BF16)
        gbu, gbd, y = pl.pallas_call(
            fwd_kernel,
            name='fwd',
            out_shape=(mat, mat, jax.ShapeDtypeStruct((NMICRO, ROWS, D), BF16)),
            in_specs=[vm, vm, hbm, hbm, hbm, hbm],
            out_specs=(hbm, hbm, hbm),
            scratch_shapes=[
                pltpu.VMEM((NF, R, D), BF16), pltpu.VMEM((NF, R, D), F32), pltpu.VMEM((NF, NZ - 1, RQ, D), F32), pltpu.VMEM((NF, RQ, D), BF16),
                dma((NF,)), dma((NF, NZ)), dma((NF, NZ - 1)), dma((NF, NZ - 1)), dma((NF, NZ)), dma((NF,)), dma((NF, NZ * NS)), dma((NF // 2, NZ)),
                dma((NCHUNK,)), dma((NCHUNK,)),
            ],
            input_output_aliases={4: 0, 5: 1},
            compiler_params=pltpu.CompilerParams(has_side_effects=True, vmem_limit_bytes=20 << 20),
        )(up_bf, down_bf, x_next, x_other, gbu, gbd)
        up_w, up_m, up_v = adamw_update(w_up[0], m_up[0], v_up[0], clip * gbu, rate)
        down_w, down_m, down_v = adamw_update(w_down[0], m_down[0], v_down[0], clip * gbd, rate)
        return (up_w[None], down_w[None], up_m[None], down_m[None], up_v[None], down_v[None], y)

    return jax.shard_map(device_step, mesh=mesh, in_specs=in_specs, out_specs=out_specs, check_vma=False)
```

```python
import functools

import jax
import jax.numpy as jnp
from jax import lax
from jax.experimental import pallas as pl
from jax.experimental.pallas import tpu as pltpu
from jax.sharding import PartitionSpec as P

ADAM_STEP = 10
BETA_ONE = 0.9
BETA_TWO = 0.95
ADAM_EPS = 1e-8
WEIGHT_DECAY = 0.1
NORM_EPS = 1e-6
ROOT_CORR = (1.0 - BETA_TWO ** ADAM_STEP) ** 0.5
DIR_SCALE = ROOT_CORR / (1.0 - BETA_ONE ** ADAM_STEP)
DIR_EPS = ADAM_EPS * ROOT_CORR
GELU_A = 0.7978845608028654
GELU_B = 0.044715
NT = (((1,), (1,)), ((), ()))
TN = (((0,), (0,)), ((), ()))
MESH = pl.DeviceIdType.MESH
F32 = jnp.float32
BF16 = jnp.bfloat16
NZ = 4
NS = 4
ROWS = 128
D = 1024
QROWS = ROWS // NZ
CH = 128
NCHUNK = 2 * D // CH
R = 64
RQ = R // NZ
NSUB = ROWS // R
NMICRO = 3
NF = NMICRO * 2 * NSUB
PRE = (11, 8, 5, 2)


def gelu_parts(x):
    t = jnp.tanh(GELU_A * (x + GELU_B * (x * x * x)))
    return 0.5 * (1.0 + t), t


def rcopy(src, dst, ssem, rsem, dev):
    return pltpu.make_async_remote_copy(src, dst, ssem, rsem, device_id=dev, device_id_type=MESH)


def axes():
    return lax.axis_index('model'), lax.axis_index('data'), lax.axis_index('stage')


def back_kernel(wu, wd, gu, gd, a_ref, dy_ref, x_ref, mn_ref,
                gbu, gbd, c_ref, xo_ref,
                wf, wub, wdb, gin, gown, fa, fg, fh, fz, gp, part, rsb, gsend, nacc, nsend, nbuf,
                wsem, osem, outsem, cs, cr, fs, fr, rs, rr, gs, gr, xs, xr, ys, yr, ns, nr):
    m, d, s = axes()
    prim = d == lax.rem(s, 2)
    sec = jnp.logical_not(prim)
    peer = (m, 1 - d, s)

    def chunk_copy(c, src):
        row = pl.ds(pl.multiple_of(lax.rem(c, D // CH) * CH, CH), CH)
        return rcopy(src.at[0, 0, row], gin.at[c // (D // CH), row], cs.at[c], cr.at[c], peer)

    def send_chunks(lo, hi):
        half = D // CH

        @pl.loop(lo, jnp.minimum(hi, half))
        def _(c):
            chunk_copy(c, gd).start()

        @pl.loop(jnp.maximum(lo, half), hi)
        def _(c):
            chunk_copy(c, gu).start()

    pre = jnp.where(s == 0, PRE[0], jnp.where(s == 1, PRE[1], jnp.where(s == 2, PRE[2], PRE[3])))
    own = pl.ds(0, ROWS)
    oth = pl.ds(ROWS, ROWS)
    fcopy = [rcopy(a_ref.at[0], fa.at[oth], fs.at[0], fr.at[0], peer)]
    fcopy += [rcopy(f.at[own], f.at[oth], fs.at[i + 1], fr.at[i + 1], peer) for i, f in enumerate((fh, fg, fz))]

    wcopies = [pltpu.make_async_copy(wu.at[0], wf.at[0], wsem.at[0]), pltpu.make_async_copy(wd.at[0], wf.at[1], wsem.at[1])]
    for cp in wcopies:
        cp.start()
    qrow = pl.ds(pl.multiple_of(m * QROWS, QROWS), QROWS)
    xcopy = rcopy(x_ref.at[:, qrow], xo_ref.at[:, qrow], xs.at[0], xr.at[0], (m, 0, s))

    @pl.when(sec)
    def _():
        @pl.when(s == 0)
        def _():
            xcopy.start()
        fcopy[0].start()
        send_chunks(0, pre)

    gcopies = [pltpu.make_async_copy(gd.at[0, 0], gown.at[0], osem.at[0]), pltpu.make_async_copy(gu.at[0, 0], gown.at[1], osem.at[1])]

    @pl.when(prim)
    def _():
        for cp in gcopies:
            cp.start()

    fa[own] = a_ref[0]
    for i, (cp, dst) in enumerate(zip(wcopies, (wub, wdb))):
        cp.wait()

        @pl.loop(0, D // CH)
        def _(c):
            row = pl.ds(pl.multiple_of(c * CH, CH), CH)
            dst[row] = wf[i, row].astype(BF16)
        if i == 0:
            pre_act = jnp.dot(a_ref[0], wub[...], preferred_element_type=F32)
            cdf, t = gelu_parts(pre_act)
            fh[own] = (pre_act * cdf).astype(BF16)
            gp[...] = cdf + pre_act * (0.5 * (1.0 - t * t) * GELU_A * (1.0 + 3.0 * GELU_B * (pre_act * pre_act)))

    @pl.when(sec)
    def _():
        fcopy[1].start()

    xfwd = [rcopy(xo_ref.at[:, qrow], xo_ref.at[:, qrow], ys.at[o - 1], yr.at[o - 1], (lax.rem(m + o, NZ), d, s)) for o in range(1, NZ)]

    @pl.when(jnp.logical_and(s == 0, d == 0))
    def _():
        xcopy.wait_recv()
        for cp in xfwd:
            cp.start()

    gsends = [rcopy(gsend, fg.at[qrow], gs.at[o], gr.at[o], (lax.rem(m + o, NZ), d, s - 1)) for o in range(NZ)]

    @pl.when(s == NS - 1)
    def _():
        fg[own] = dy_ref[...]

    @pl.when(s < NS - 1)
    def _():
        for cp in gsends:
            cp.wait_recv()

    @pl.when(sec)
    def _():
        fcopy[2].start()

    grad_hid = lax.dot_general(fg[own], wdb[...], NT, preferred_element_type=F32)
    fz[own] = (gp[...] * grad_hid).astype(BF16)

    @pl.when(s > 0)
    def _():
        part[...] = lax.dot_general(fz[own], wub[...], NT, preferred_element_type=F32)
        rcp = []
        for o in range(1, NZ):
            to = lax.rem(m + o, NZ)
            row = pl.ds(pl.multiple_of(to * QROWS, QROWS), QROWS)
            rcp.append(rcopy(part.at[row], rsb.at[o - 1], rs.at[o - 1], rr.at[o - 1], (to, d, s)))
        for cp in rcp:
            cp.start()
        total = part[qrow]
        for o, cp in enumerate(rcp):
            cp.wait_recv()
            total = total + rsb[o]
        gsend[...] = (fg[qrow].astype(F32) + total).astype(BF16)
        for cp in gsends:
            cp.start()
        for cp in rcp:
            cp.wait_send()

    @pl.when(sec)
    def _():
        fcopy[3].start()
        send_chunks(pre, NCHUNK)

    @pl.when(s > 0)
    def _():
        for cp in gsends:
            cp.wait_send()

    slot = s * NZ + m

    @pl.when(prim)
    def _():
        for cp in gcopies:
            cp.wait()
        for cp in fcopy:
            cp.wait_recv()
        nacc[...] = jnp.zeros_like(nacc)
        for half, (lhs, rhs, src, out) in enumerate(((fh, fg, gd, gbd), (fa, fz, gu, gbu))):
            @pl.loop(0, D // CH)
            def _(c):
                row = pl.ds(pl.multiple_of(c * CH, CH), CH)
                grad = lax.dot_general(lhs[:, row], rhs[...], TN, preferred_element_type=F32)
                chunk_copy(half * (D // CH) + c, src).wait_recv()
                bar = (gown[half, row] + gin[half, row] + grad) * 0.5
                gown[half, row] = bar
                nacc[...] += jnp.sum((bar * bar).reshape(CH // 8, 8, D), axis=0)
                pltpu.make_async_copy(gown.at[half, row], out.at[row], outsem.at[half * (D // CH) + c]).start()
        tot = nacc[:, 0:128]
        for i in range(1, D // 128):
            tot = tot + nacc[:, i * 128:(i + 1) * 128]
        nsend[...] = tot
        nbuf[slot] = tot

    def ncopy(to, sl):
        return rcopy(nsend, nbuf.at[sl], ns.at[to], nr.at[sl], (to // (2 * NS), lax.rem(to // NS, 2), lax.rem(to, NS)))

    me = (m * 2 + d) * NS + s

    @pl.when(prim)
    def _():
        @pl.loop(0, NZ * 2 * NS)
        def _(to):
            @pl.when(to != me)
            def _():
                ncopy(to, slot).start()

    @pl.loop(0, NZ * NS)
    def _(i):
        @pl.when(jnp.logical_or(sec, i != slot))
        def _():
            ncopy(0, i).wait_recv()

    total = jnp.sum(jnp.sum(nbuf[...], axis=0), keepdims=True)
    c_ref[...] = jnp.broadcast_to(jnp.minimum(1.0, mn_ref[0] / (jnp.sqrt(total) + NORM_EPS)), c_ref.shape)

    @pl.when(prim)
    def _():
        @pl.loop(0, NZ * 2 * NS)
        def _(to):
            @pl.when(to != me)
            def _():
                ncopy(to, slot).wait_send()
        for half, out in enumerate((gbd, gbu)):
            @pl.loop(0, D // CH)
            def _(c):
                row = pl.ds(pl.multiple_of(c * CH, CH), CH)
                pltpu.make_async_copy(gown.at[half, row], out.at[row], outsem.at[half * (D // CH) + c]).wait()

    @pl.when(sec)
    def _():
        for cp in fcopy:
            cp.wait_send()

        @pl.loop(0, NCHUNK)
        def _(c):
            chunk_copy(c, gd).wait_send()

    @pl.when(jnp.logical_and(s == 0, d == 0))
    def _():
        for cp in xfwd:
            cp.wait()

    @pl.when(jnp.logical_and(s == 0, d == 1))
    def _():
        xcopy.wait_send()


def fwd_kernel(w1, w2, x_ref, xo_ref, gbu_in, gbd_in, gbu, gbd, y_ref,
               inb, part, rsb, osend, isem, ir, rs, rr, os, yo, ys, yr, yt, yq, cs, cr):
    m, d, s = axes()
    prim = d == lax.rem(s, 2)
    sec = jnp.logical_not(prim)
    peer = (m, 1 - d, s)
    half = D // CH
    oq = pl.ds(pl.multiple_of(m * RQ, RQ), RQ)

    def bulk(c, ref):
        row = pl.ds(pl.multiple_of(lax.rem(c, half) * CH, CH), CH)
        return rcopy(ref.at[row], ref.at[row], cs.at[c], cr.at[c], peer)

    def send_chunks(lo, hi):
        @pl.loop(lo, jnp.minimum(hi, half))
        def _(c):
            bulk(c, gbd).start()

        @pl.loop(jnp.maximum(lo, half), hi)
        def _(c):
            bulk(c, gbu).start()

    up = 1 + 2 * s

    def goal(k):
        return up + (NCHUNK - up) * k // NF

    def where_is(k):
        return k // (2 * NSUB), lax.rem(k // NSUB, 2), lax.rem(k, NSUB)

    def in_copy(k, o):
        return rcopy(osend.at[k], inb.at[k, oq], os.at[k, o], ir.at[k, o], (lax.rem(m + o, NZ), lax.rem(s + 1, 2), s + 1))

    def rs_copy(k, o):
        to = lax.rem(m + o, NZ)
        row = pl.ds(pl.multiple_of(to * RQ, RQ), RQ)
        return rcopy(part.at[k, row], rsb.at[k, o - 1], rs.at[k, o - 1], rr.at[k, o - 1], (to, d, s))

    def y_at(kk, q):
        i, sub = kk // NSUB, lax.rem(kk, NSUB)
        return y_ref.at[i, pl.ds(pl.multiple_of(sub * R + q * RQ, RQ), RQ)]

    def y_out(k, xx):
        i, r, sub = where_is(k)
        kk = i * NSUB + sub
        return rcopy(osend.at[k], y_at(kk, m), yo.at[k, xx], yr.at[kk, 0], (m, r, 2 * xx + 1 - r))

    def y_ring(kk, o):
        return rcopy(y_at(kk, m), y_at(kk, m), ys.at[kk, o], yr.at[kk, o], (lax.rem(m + o, NZ), d, s))

    def y_mate(kk, o):
        q = lax.rem(m - o + NZ, NZ)
        return rcopy(y_at(kk, q), y_at(kk, q), yt.at[kk, o], yq.at[kk, o], (m, d, s + 1 - 2 * lax.rem(s, 2)))

    def compute(k):
        @pl.when(s > 0)
        def _():
            for o in range(NZ):
                in_copy(k, o).wait_recv()
        pre_act = jnp.dot(inb[k], w1[...], preferred_element_type=F32)
        hid = (pre_act * gelu_parts(pre_act)[0]).astype(BF16)
        part[k] = jnp.dot(hid, w2[...], preferred_element_type=F32)
        for o in range(1, NZ):
            rs_copy(k, o).start()

    def finish(k):
        total = part[k, oq]
        for o in range(1, NZ):
            rs_copy(k, o).wait_recv()
            total = total + rsb[k, o - 1]
        osend[k] = (inb[k, oq].astype(F32) + total).astype(BF16)

        @pl.when(s < NS - 1)
        def _():
            for o in range(NZ):
                in_copy(k, o).start()

        @pl.when(s == NS - 1)
        def _():
            for xx in range(2):
                y_out(k, xx).start()

    def in_local(k, src, row, i):
        return pltpu.make_async_copy(src.at[i, row], inb.at[k], isem.at[k])

    @pl.when(prim)
    def _():
        @pl.when(s == 0)
        def _():
            for step in ('start', 'wait'):
                for k in range(NF):
                    i, r, sub = k // (2 * NSUB), (k // NSUB) % 2, k % NSUB
                    getattr(in_local(k, (x_ref, xo_ref)[r], pl.ds(sub * R, R), i), step)()
        send_chunks(0, up)
        compute(0)

        @pl.loop(1, NF)
        def _(k):
            compute(k)
            finish(k - 1)
            send_chunks(goal(k - 1), goal(k))
        finish(NF - 1)
        send_chunks(goal(NF - 1), NCHUNK)

    @pl.when(sec)
    def _():
        @pl.loop(0, NF // 2)
        def _(kk):
            y_ring(kk, 0).wait_recv()
            for o in range(1, NZ):
                y_ring(kk, o).start()
            y_mate(kk, 0).start()
            for o in range(1, NZ):
                y_ring(kk, o).wait_recv()
                y_mate(kk, o).start()

    @pl.when(prim)
    def _():
        @pl.loop(0, NF // 2)
        def _(kk):
            for o in range(NZ):
                y_mate(kk, o).wait_recv()

    @pl.when(sec)
    def _():
        @pl.loop(0, NCHUNK)
        def _(c):
            bulk(c, gbd).wait_recv()

        @pl.loop(0, NF // 2)
        def _(kk):
            for o in range(1, NZ):
                y_ring(kk, o).wait_send()
            for o in range(NZ):
                y_mate(kk, o).wait_send()

    @pl.when(prim)
    def _():
        @pl.loop(0, NF)
        def _(k):
            for o in range(1, NZ):
                rs_copy(k, o).wait_send()

            @pl.when(s < NS - 1)
            def _():
                for o in range(NZ):
                    in_copy(k, o).wait_send()

            @pl.when(s == NS - 1)
            def _():
                for xx in range(2):
                    y_out(k, xx).wait_send()

        @pl.loop(0, NCHUNK)
        def _(c):
            bulk(c, gbd).wait_send()


def adamw_update(weight, moment_one, moment_two, grad_step, step_rate):
    mom_new = BETA_ONE * moment_one + (1.0 - BETA_ONE) * grad_step
    sec_new = BETA_TWO * moment_two + (1.0 - BETA_TWO) * grad_step * grad_step
    direction = (DIR_SCALE * mom_new) / (jnp.sqrt(sec_new) + DIR_EPS)
    weight_new = weight - step_rate * (direction + WEIGHT_DECAY * weight)
    return weight_new, mom_new, sec_new


def solution(mesh):
    up_spec = P('stage', None, 'model')
    down_spec = P('stage', 'model', None)
    row_spec = P(None, 'data', None)
    in_specs = (up_spec, down_spec, up_spec, down_spec, up_spec, down_spec, P('data', 'stage', None, 'model'), P('data', 'stage', 'model', None), P('stage', 'data', None), P('data', None), row_spec, P(None), P(None))
    out_specs = (up_spec, down_spec, up_spec, down_spec, up_spec, down_spec, row_spec)
    hbm = pl.BlockSpec(memory_space=pl.ANY)
    vm = pl.BlockSpec(memory_space=pltpu.VMEM)
    sm = pl.BlockSpec(memory_space=pltpu.SMEM)
    dma = pltpu.SemaphoreType.DMA
    mat = jax.ShapeDtypeStruct((D, D), F32)

    def device_step(w_up, w_down, m_up, m_down, v_up, v_down, g_up, g_down, acts_last, grad_out, x_next, learn_rate, max_norm):
        gbu, gbd, clip, x_other = pl.pallas_call(
            back_kernel,
            name='back',
            out_shape=(mat, mat, jax.ShapeDtypeStruct((8, 128), F32), jax.ShapeDtypeStruct((NMICRO, ROWS, D), BF16)),
            in_specs=[hbm, hbm, hbm, hbm, vm, vm, hbm, sm],
            out_specs=(hbm, hbm, vm, hbm),
            scratch_shapes=[
                pltpu.VMEM((2, D, D), F32), pltpu.VMEM((D, D), BF16), pltpu.VMEM((D, D), BF16),
                pltpu.VMEM((2, D, D), F32), pltpu.VMEM((2, D, D), F32),
                *[pltpu.VMEM((2 * ROWS, D), BF16)] * 4,
                pltpu.VMEM((ROWS, D), F32), pltpu.VMEM((ROWS, D), F32), pltpu.VMEM((NZ - 1, QROWS, D), F32),
                pltpu.VMEM((QROWS, D), BF16), pltpu.VMEM((8, D), F32), pltpu.VMEM((8, 128), F32), pltpu.VMEM((NZ * NS, 8, 128), F32),
                dma((2,)), dma((2,)), dma((NCHUNK,)), dma((NCHUNK,)), dma((NCHUNK,)), dma((4,)), dma((4,)),
                dma((NZ - 1,)), dma((NZ - 1,)), dma((NZ,)), dma((NZ,)), dma((1,)), dma((1,)), dma((NZ - 1,)), dma((NZ - 1,)),
                dma((NZ * 2 * NS,)), dma((NZ * NS,)),
            ],
            compiler_params=pltpu.CompilerParams(has_side_effects=True, vmem_limit_bytes=48 << 20),
        )(w_up, w_down, g_up, g_down, acts_last, grad_out, x_next, max_norm)
        clip = clip[0, 0]
        rate = learn_rate[0]
        up_bf = adamw_update(w_up[0], m_up[0], v_up[0], clip * gbu, rate)[0].astype(BF16)
        down_bf = adamw_update(w_down[0], m_down[0], v_down[0], clip * gbd, rate)[0].astype(BF16)
        gbu, gbd, y = pl.pallas_call(
            fwd_kernel,
            name='fwd',
            out_shape=(mat, mat, jax.ShapeDtypeStruct((NMICRO, ROWS, D), BF16)),
            in_specs=[vm, vm, hbm, hbm, hbm, hbm],
            out_specs=(hbm, hbm, vm),
            scratch_shapes=[
                pltpu.VMEM((NF, R, D), BF16), pltpu.VMEM((NF, R, D), F32), pltpu.VMEM((NF, NZ - 1, RQ, D), F32), pltpu.VMEM((NF, RQ, D), BF16),
                dma((NF,)), dma((NF, NZ)), dma((NF, NZ - 1)), dma((NF, NZ - 1)), dma((NF, NZ)), dma((NF, 2)), *[dma((NF // 2, NZ))] * 4,
                dma((NCHUNK,)), dma((NCHUNK,)),
            ],
            input_output_aliases={4: 0, 5: 1},
            compiler_params=pltpu.CompilerParams(has_side_effects=True, vmem_limit_bytes=20 << 20),
        )(up_bf, down_bf, x_next, x_other, gbu, gbd)
        up_w, up_m, up_v = adamw_update(w_up[0], m_up[0], v_up[0], clip * gbu, rate)
        down_w, down_m, down_v = adamw_update(w_down[0], m_down[0], v_down[0], clip * gbd, rate)
        return (up_w[None], down_w[None], up_m[None], down_m[None], up_v[None], down_v[None], y)

    return jax.shard_map(device_step, mesh=mesh, in_specs=in_specs, out_specs=out_specs, check_vma=False)
```
